8 devices in a mesh: dp: 2 (over z, y), col: 2 (over x), fsdp: 2 (over core).
Axes of the slice: x: 2, y: 2, z: 1, core: 2. Of those that a mesh axis runs over, the one named last changes fastest.
Arguments:
- x_act: bfloat16 [32768, 576], P(('dp', 'col', 'fsdp'))
- dy_out: bfloat16 [32768, 576], P(('dp', 'col', 'fsdp'))
- w_gate: bfloat16 [576, 1536], P(None, ('col', 'fsdp'))
- w_up: bfloat16 [576, 1536], P(None, ('col', 'fsdp'))
- w_down: bfloat16 [1536, 576], P(('col', 'fsdp'))
- v_gate: bfloat16 [576, 1536], P(None, ('col', 'fsdp'))
- v_up: bfloat16 [576, 1536], P(None, ('col', 'fsdp'))
- v_down: bfloat16 [1536, 576], P(('col', 'fsdp'))
- g_next: float32 [8, 3, 576, 1536], P(('dp', 'col', 'fsdp'))
Outputs:
- output 1: bfloat16 [32768, 576], P(('dp', 'col', 'fsdp'))
- output 2: float32 [3, 576, 1536], P(None, None, ('col', 'fsdp'))
- output 3: float32 [8, 3, 576, 1536], P(('dp', 'col', 'fsdp'))
- output 4: bfloat16 [576, 1536], replicated
- output 5: bfloat16 [576, 1536], replicated
- output 6: bfloat16 [1536, 576], replicated
All inputs are finite; a program needn't handle non-finite values.
Results may differ from the reference program's by a relative error of at most 0.00911928.
Values are sent between devices in bfloat16 or wider.
A program may use at most 1 GiB of HBM per device.

```python
import jax
import jax.numpy as jnp
from jax import lax

D_MODEL = 576
D_FF = 1536
TOKENS_DEV = 4096
N_DEVICES = 8


def draw_normal(key, shape, scaling):
    return jax.random.normal(key, shape, jnp.float32) * scaling


def setup_inputs(seed: int = 0) -> dict:
    keys = jax.random.split(jax.random.key(seed), 9)
    all_rows = N_DEVICES * TOKENS_DEV
    model_scale = D_MODEL ** -0.5
    hidden_scale = D_FF ** -0.5
    return {
        'x_act': draw_normal(keys[0], (all_rows, D_MODEL), 1.0).astype(jnp.bfloat16),
        'dy_out': draw_normal(keys[1], (all_rows, D_MODEL), 1.0).astype(jnp.bfloat16),
        'w_gate': draw_normal(keys[2], (D_MODEL, D_FF), model_scale).astype(jnp.bfloat16),
        'w_up': draw_normal(keys[3], (D_MODEL, D_FF), model_scale).astype(jnp.bfloat16),
        'w_down': draw_normal(keys[4], (D_FF, D_MODEL), hidden_scale).astype(jnp.bfloat16),
        'v_gate': draw_normal(keys[5], (D_MODEL, D_FF), model_scale).astype(jnp.bfloat16),
        'v_up': draw_normal(keys[6], (D_MODEL, D_FF), model_scale).astype(jnp.bfloat16),
        'v_down': draw_normal(keys[7], (D_FF, D_MODEL), hidden_scale).astype(jnp.bfloat16),
        'g_next': draw_normal(keys[8], (N_DEVICES, 3, D_MODEL, D_FF), 1.0),
    }


def reference(x_act, dy_out, w_gate, w_up, w_down, v_gate, v_up, v_down, g_next):
    x_dev = x_act.reshape(N_DEVICES, TOKENS_DEV, D_MODEL)
    dy_dev = dy_out.reshape(N_DEVICES, TOKENS_DEV, D_MODEL)

    def one_device(operands):
        x_loc, dy_loc = operands
        pre_gate = jnp.dot(x_loc, w_gate, preferred_element_type=jnp.float32)
        pre_up = jnp.dot(x_loc, w_up, preferred_element_type=jnp.float32)
        sig_gate = jax.nn.sigmoid(pre_gate)
        act_gate = pre_gate * sig_gate
        hidden = (act_gate * pre_up).astype(jnp.bfloat16)
        d_hidden = jnp.dot(dy_loc, w_down.T, preferred_element_type=jnp.float32)
        d_gate = (d_hidden * pre_up * sig_gate * (1.0 + pre_gate * (1.0 - sig_gate))).astype(jnp.bfloat16)
        d_up = (d_hidden * act_gate).astype(jnp.bfloat16)
        dx_loc = (jnp.dot(d_gate, w_gate.T, preferred_element_type=jnp.float32)
                  + jnp.dot(d_up, w_up.T, preferred_element_type=jnp.float32)).astype(jnp.bfloat16)
        grad_gate = jnp.dot(x_loc.T, d_gate, preferred_element_type=jnp.float32)
        grad_up = jnp.dot(x_loc.T, d_up, preferred_element_type=jnp.float32)
        grad_down_t = jnp.dot(dy_loc.T, hidden, preferred_element_type=jnp.float32)
        return dx_loc, jnp.stack([grad_gate, grad_up, grad_down_t])

    dx_dev, dw_local = lax.map(one_device, (x_dev, dy_dev))
    dx_in = dx_dev.reshape(N_DEVICES * TOKENS_DEV, D_MODEL)
    dw_next = jnp.sum(g_next.astype(jnp.bfloat16).astype(jnp.float32), axis=0)
    return dx_in, dw_next, dw_local, v_gate, v_up, v_down
```

```python
import functools
import jax
import jax.numpy as jnp
from jax import lax
from jax.experimental import pallas as pl
from jax.experimental.pallas import tpu as pltpu
from jax.sharding import PartitionSpec as P

ALL_AXES = ('dp', 'col', 'fsdp')
FSDP_AXES = ('col', 'fsdp')
D, F, T = 576, 1536, 4096
FH = F // 2
TT = 512
NT = T // TT
F32, BF16 = jnp.float32, jnp.bfloat16


def dot(a, b, ca, cb):
    return lax.dot_general(a, b, (((ca,), (cb,)), ((), ())), preferred_element_type=F32)


def tile_step(i, first, x_ref, dy_ref, w13, w2, dxt, dw13, dw2):
    x, dy = x_ref[i], dy_ref[i]
    ab = dot(x, w13[...], 1, 0)
    dh = dot(dy, w2[...], 1, 1)
    a, b = ab[:, :FH], ab[:, FH:]
    s = 0.5 * jnp.tanh(0.5 * a) + 0.5
    act = a * s
    h = (act * b).astype(BF16)
    dg = (dh * b * s * (1.0 + a * (1.0 - s))).astype(BF16)
    du = (dh * act).astype(BF16)
    dgu = jnp.concatenate([dg, du], axis=1)
    dxt_new = dot(w13[...], dgu, 1, 1)
    if first:
        dxt[i] = dxt_new
    else:
        dxt[i] = dxt[i] + dxt_new
    dw13[...] += dot(x, dgu, 0, 0)
    dw2[...] += dot(dy, h, 0, 0)


def kernel(x_hbm, dy_hbm, w1, w3, w2, dx_hbm, dw_hbm, xv, dyv, w13v, w2v, dxt, dw13, dw2, dxo, sems, osem):
    cx = pltpu.make_async_copy(x_hbm, xv, sems.at[0])
    cy = pltpu.make_async_copy(dy_hbm, dyv, sems.at[1])
    cx.start()
    cy.start()
    cx.wait()
    cy.wait()
    for p in range(2):
        lo = p * FH
        cw = [pltpu.make_async_copy(w1.at[:, pl.ds(lo, FH)], w13v.at[:, pl.ds(0, FH)], sems.at[2]),
              pltpu.make_async_copy(w3.at[:, pl.ds(lo, FH)], w13v.at[:, pl.ds(FH, FH)], sems.at[3]),
              pltpu.make_async_copy(w2.at[pl.ds(lo, FH), :], w2v, sems.at[4])]
        for c in cw:
            c.start()
        for c in cw:
            c.wait()
        dw13[...] = jnp.zeros_like(dw13)
        dw2[...] = jnp.zeros_like(dw2)

        @pl.loop(0, NT)
        def _(i):
            tile_step(i, p == 0, xv, dyv, w13v, w2v, dxt, dw13, dw2)
            if p == 1:
                @pl.when(i > 0)
                def _():
                    pltpu.make_async_copy(dxo, dx_hbm.at[i - 1], osem).wait()
                dxo[...] = dxt[i].astype(BF16).T
                pltpu.make_async_copy(dxo, dx_hbm.at[i], osem).start()
        co = [pltpu.make_async_copy(dw13.at[:, pl.ds(0, FH)], dw_hbm.at[0, :, pl.ds(lo, FH)], sems.at[2]),
              pltpu.make_async_copy(dw13.at[:, pl.ds(FH, FH)], dw_hbm.at[1, :, pl.ds(lo, FH)], sems.at[3]),
              pltpu.make_async_copy(dw2, dw_hbm.at[2, :, pl.ds(lo, FH)], sems.at[4])]
        for c in co:
            c.start()
        for c in co:
            c.wait()
    pltpu.make_async_copy(dxo, dx_hbm.at[NT - 1], osem).wait()


def mlp(x, dy, w1, w3, w2):
    anys = pl.BlockSpec(memory_space=pl.ANY)
    dx, dw = pl.pallas_call(
        kernel,
        out_shape=[jax.ShapeDtypeStruct((NT, TT, D), BF16), jax.ShapeDtypeStruct((3, D, F), F32)],
        in_specs=[anys] * 5, out_specs=[anys] * 2,
        scratch_shapes=[
            pltpu.VMEM((NT, TT, D), BF16), pltpu.VMEM((NT, TT, D), BF16),
            pltpu.VMEM((D, F), BF16), pltpu.VMEM((FH, D), BF16),
            pltpu.VMEM((NT, D, TT), F32), pltpu.VMEM((D, F), F32), pltpu.VMEM((D, FH), F32),
            pltpu.VMEM((TT, D), BF16),
            pltpu.SemaphoreType.DMA((5,)), pltpu.SemaphoreType.DMA,
        ],
        compiler_params=pltpu.CompilerParams(vmem_limit_bytes=67043328),
        cost_estimate=pl.CostEstimate(flops=8 * 2 * T * D * F, bytes_accessed=40 * 2**20, transcendentals=T * F),
        name='mlp_bwd',
    )(x.reshape(NT, TT, D), dy.reshape(NT, TT, D), w1, w3, w2)
    return dx.reshape(T, D), dw


def solution(mesh):
    def device_step(x_loc, dy_loc, w_gate, w_up, w_down, v_gate, v_up, v_down, g_next):
        gate_full = lax.all_gather(w_gate, FSDP_AXES, axis=1, tiled=True)
        up_full = lax.all_gather(w_up, FSDP_AXES, axis=1, tiled=True)
        down_full = lax.all_gather(w_down, FSDP_AXES, axis=0, tiled=True)
        v_gate_full = lax.all_gather(v_gate, FSDP_AXES, axis=1, tiled=True)
        v_up_full = lax.all_gather(v_up, FSDP_AXES, axis=1, tiled=True)
        v_down_full = lax.all_gather(v_down, FSDP_AXES, axis=0, tiled=True)
        grad_shard = lax.psum_scatter(g_next[0].astype(jnp.bfloat16), FSDP_AXES, scatter_dimension=2, tiled=True)
        other = lax.ppermute(grad_shard, 'dp', [(0, 1), (1, 0)])
        grad_next = grad_shard.astype(F32) + other.astype(F32)
        dx_loc, grad_local = mlp(x_loc, dy_loc, gate_full, up_full, down_full)
        return dx_loc, grad_next, grad_local[None], v_gate_full, v_up_full, v_down_full

    row_spec = P(ALL_AXES, None)
    col_shard = P(None, FSDP_AXES)
    row_shard = P(FSDP_AXES, None)
    dev_spec = P(ALL_AXES, None, None, None)
    return jax.shard_map(
        device_step, mesh=mesh,
        in_specs=(row_spec, row_spec, col_shard, col_shard, row_shard, col_shard, col_shard, row_shard, dev_spec),
        out_specs=(row_spec, P(None, None, FSDP_AXES), dev_spec, P(), P(), P()),
        check_vma=False)
```
